8 devices in a mesh: member: 1 (over z), lon: 2 (over y), lat: 4 (over x, core).
Axes of the slice: x: 2, y: 2, z: 1, core: 2. Of those that a mesh axis runs over, the one named last changes fastest.
Arguments:
- grid_field: float32 [6, 384, 180, 360], P('member', None, 'lat', 'lon')
- mix_weight: bfloat16 [180, 384, 384, 2], replicated
Outputs:
- output: float32 [6, 384, 180, 360], P('member', None, 'lat', 'lon')
All inputs are finite; a program needn't handle non-finite values.
Results may differ from the reference program's by a relative error of at most 0.00404289.
Values are sent between devices in bfloat16 or wider.
A program may use at most 1 GiB of HBM per device.

```python
import math
import jax
import jax.numpy as jnp
from jax import lax

BATCH_SIZE = 6
CHANNELS = 384
LAT_ROWS = 180
MAX_DEGREE = 180
LON_POINTS = 2 * LAT_ROWS


def legendre_table(m_vals, colatitude, n_deg):
    cos_t = jnp.cos(colatitude)[None, :]
    m_int = m_vals[:, None]
    m_col = m_int.astype(jnp.float32)
    deg_all = jnp.arange(1, n_deg + 1).astype(jnp.float32)
    log_steps = 0.5 * jnp.log((2.0 * deg_all + 1.0) / (2.0 * deg_all))
    cum_log = jnp.concatenate([jnp.zeros((1,), jnp.float32), jnp.cumsum(log_steps)])
    log_diag = 0.5 * math.log(0.5) + cum_log[m_vals][:, None] + m_col * jnp.log(jnp.sin(colatitude))[None, :]

    def degree_step(carry, degree):
        prev_one, prev_two, log_scale = carry
        deg_f = degree.astype(jnp.float32)
        at_start = m_int == degree
        is_above = m_int < degree
        coef_a = jnp.sqrt((4.0 * deg_f * deg_f - 1.0) / jnp.maximum(deg_f * deg_f - m_col * m_col, 1.0))
        coef_b = jnp.sqrt(jnp.maximum((deg_f - 1.0) ** 2 - m_col * m_col, 0.0) / jnp.maximum(4.0 * (deg_f - 1.0) ** 2 - 1.0, 1.0))
        rec_value = coef_a * (cos_t * prev_one - coef_b * prev_two)
        renorm = jnp.maximum(jnp.abs(rec_value), 1.0)
        next_one = jnp.where(at_start, 1.0, jnp.where(is_above, rec_value / renorm, 0.0))
        next_two = jnp.where(is_above, prev_one / renorm, 0.0)
        next_scale = jnp.where(at_start, log_diag, jnp.where(is_above, log_scale + jnp.log(renorm), 0.0))
        out_value = jnp.where(at_start | is_above, next_one * jnp.exp(next_scale), 0.0)
        return (next_one, next_two, next_scale), out_value

    zero_state = jnp.zeros((m_vals.shape[0], colatitude.shape[0]), jnp.float32)
    return lax.scan(degree_step, (zero_state, zero_state, zero_state), jnp.arange(n_deg))[1]


def fejer_weights(colatitude, n_lat):
    harmonic = jnp.arange(1, n_lat // 2 + 1).astype(jnp.float32)
    series = jnp.cos(2.0 * colatitude[:, None] * harmonic[None, :]) / (4.0 * harmonic * harmonic - 1.0)
    return (2.0 / n_lat) * (1.0 - 2.0 * jnp.sum(series, axis=1))


def dft_tables(n_lon, n_deg):
    lon_index = jnp.arange(n_lon)
    deg_index = jnp.arange(n_deg)
    fwd_angle = ((lon_index[:, None] * deg_index[None, :]) % n_lon).astype(jnp.float32) * (2.0 * math.pi / n_lon)
    fwd_table = jnp.concatenate([jnp.cos(fwd_angle), -jnp.sin(fwd_angle)], axis=1).astype(jnp.bfloat16)
    inv_angle = ((deg_index[:, None] * lon_index[None, :]) % n_lon).astype(jnp.float32) * (2.0 * math.pi / n_lon)
    weight_m = jnp.where(deg_index == 0, 1.0, 2.0)[:, None]
    inv_table = jnp.concatenate([weight_m * jnp.cos(inv_angle), -weight_m * jnp.sin(inv_angle)], axis=0).astype(jnp.bfloat16)
    return fwd_table, inv_table


def setup_inputs(seed: int = 0, part: int = 0) -> dict:
    part_key = jax.random.fold_in(jax.random.key(seed), part)
    noise_key, smooth_key = jax.random.split(part_key)
    colatitude = (jnp.arange(LAT_ROWS).astype(jnp.float32) + 0.5) * (math.pi / LAT_ROWS)
    longitude = jnp.arange(LON_POINTS).astype(jnp.float32) * (2.0 * math.pi / LON_POINTS)
    sin_lat = jnp.sin(colatitude)[:, None]
    smooth_basis = jnp.stack([jnp.broadcast_to(jnp.cos(colatitude)[:, None], (LAT_ROWS, LON_POINTS)), sin_lat * jnp.cos(longitude)[None, :], sin_lat * jnp.sin(longitude)[None, :]])
    smooth_amp = jax.random.normal(smooth_key, (BATCH_SIZE, CHANNELS, 3), jnp.float32)
    noise_part = jax.random.normal(noise_key, (BATCH_SIZE, CHANNELS, LAT_ROWS, LON_POINTS), jnp.float32)
    grid_field = noise_part + jnp.einsum('bcs,skj->bckj', smooth_amp, smooth_basis)
    weight_key = jax.random.key(seed + 1)
    mix_weight = (jax.random.normal(weight_key, (MAX_DEGREE, CHANNELS, CHANNELS, 2), jnp.float32) * CHANNELS ** -0.5).astype(jnp.bfloat16)
    return {'grid_field': grid_field, 'mix_weight': mix_weight}


def reference(grid_field, mix_weight):
    fwd_table, inv_table = dft_tables(LON_POINTS, MAX_DEGREE)
    colatitude = (jnp.arange(LAT_ROWS).astype(jnp.float32) + 0.5) * (math.pi / LAT_ROWS)
    leg_table = legendre_table(jnp.arange(MAX_DEGREE), colatitude, MAX_DEGREE)
    leg_fwd = (leg_table * (fejer_weights(colatitude, LAT_ROWS) / LON_POINTS)).astype(jnp.bfloat16).astype(jnp.float32)
    leg_inv = leg_table.astype(jnp.bfloat16).astype(jnp.float32)
    weight_f = mix_weight.astype(jnp.float32)
    weight_re = weight_f[..., 0]
    weight_im = weight_f[..., 1]

    def layer_sample(sample_field):
        field_bf = sample_field.astype(jnp.bfloat16)
        fourier = jnp.dot(field_bf.reshape(CHANNELS * LAT_ROWS, LON_POINTS), fwd_table, preferred_element_type=jnp.float32)
        fourier = fourier.astype(jnp.bfloat16).astype(jnp.float32).reshape(CHANNELS, LAT_ROWS, 2, MAX_DEGREE)
        spec_coef = jnp.einsum('ckrm,lmk->clrm', fourier, leg_fwd).astype(jnp.bfloat16).astype(jnp.float32)
        coef_re = spec_coef[:, :, 0, :]
        coef_im = spec_coef[:, :, 1, :]
        mixed_re = jnp.einsum('ilm,lio->olm', coef_re, weight_re) - jnp.einsum('ilm,lio->olm', coef_im, weight_im)
        mixed_im = jnp.einsum('ilm,lio->olm', coef_im, weight_re) + jnp.einsum('ilm,lio->olm', coef_re, weight_im)
        mixed_coef = jnp.stack([mixed_re, mixed_im], axis=2).astype(jnp.bfloat16).astype(jnp.float32)
        spec_grid = jnp.einsum('clrm,lmk->ckrm', mixed_coef, leg_inv).astype(jnp.bfloat16)
        grid_out = jnp.dot(spec_grid.reshape(CHANNELS * LAT_ROWS, 2 * MAX_DEGREE), inv_table, preferred_element_type=jnp.float32)
        grid_out = grid_out.astype(jnp.bfloat16).astype(jnp.float32).reshape(CHANNELS, LAT_ROWS, LON_POINTS)
        return sample_field + jax.nn.gelu(grid_out, approximate=False)

    return lax.map(layer_sample, grid_field)
```

```python
import functools
import math
import numpy as np
import jax
import jax.numpy as jnp
from jax import lax
from jax.experimental import pallas as pl
from jax.experimental.pallas import tpu as pltpu
from jax.sharding import PartitionSpec as P

BF = jnp.bfloat16
F32 = jnp.float32
LANE = 128


def legendre_table(n_lat, n_deg):
    colat = (np.arange(n_lat) + 0.5) * (math.pi / n_lat)
    cos_t = np.cos(colat)[None, :]
    m_int = np.arange(n_deg)[:, None]
    m_col = m_int.astype(np.float64)
    deg = np.arange(1, n_deg + 1).astype(np.float64)
    cum_log = np.concatenate([np.zeros(1), np.cumsum(0.5 * np.log((2 * deg + 1) / (2 * deg)))])
    log_diag = 0.5 * math.log(0.5) + cum_log[m_int] + m_col * np.log(np.sin(colat))[None, :]
    one = np.zeros((n_deg, n_lat))
    two = np.zeros((n_deg, n_lat))
    scale = np.zeros((n_deg, n_lat))
    table = np.zeros((n_deg, n_deg, n_lat))
    for l in range(n_deg):
        start = m_int == l
        above = m_int < l
        coef_a = np.sqrt((4.0 * l * l - 1.0) / np.maximum(l * l - m_col * m_col, 1.0)) if l else np.ones_like(m_col)
        coef_b = np.sqrt(np.maximum((l - 1.0) ** 2 - m_col * m_col, 0.0) / max(4.0 * (l - 1.0) ** 2 - 1.0, 1.0))
        value = coef_a * (cos_t * one - coef_b * two)
        renorm = np.maximum(np.abs(value), 1.0)
        new_one = np.where(start, 1.0, np.where(above, value / renorm, 0.0))
        two = np.where(above, one / renorm, 0.0)
        scale = np.where(start, log_diag, np.where(above, scale + np.log(renorm), 0.0))
        one = new_one
        table[l] = np.where(start | above, one * np.exp(scale), 0.0)
    return table


def fejer_weights(n_lat):
    colat = (np.arange(n_lat) + 0.5) * (math.pi / n_lat)
    n = np.arange(1, n_lat // 2 + 1).astype(np.float64)
    series = np.cos(2.0 * colat[:, None] * n[None, :]) / (4.0 * n * n - 1.0)
    return (2.0 / n_lat) * (1.0 - 2.0 * series.sum(axis=1))


def build_tables(n_lat, n_lon, n_deg, lat_devs, lon_devs, row_pad):
    rows = n_lat // lat_devs
    cols = n_lon // lon_devs
    m_per = n_deg // lat_devs
    leg = legendre_table(n_lat, n_deg)
    leg_w = leg * (fejer_weights(n_lat) / n_lon)[None, None, :]
    angle = (2.0 * math.pi / n_lon) * ((np.arange(n_deg)[:, None] * np.arange(n_lon)[None, :]) % n_lon)
    weight = np.where(np.arange(n_deg) == 0, 1.0, 2.0)[:, None]
    fwd = np.stack([np.cos(angle), -np.sin(angle)], axis=1)
    inv = np.stack([weight * np.cos(angle), -weight * np.sin(angle)], axis=1)
    t_fwd = np.zeros((lat_devs, lon_devs, lon_devs, 2 * n_deg, cols))
    t_inv = np.zeros((lat_devs, lon_devs, lon_devs, cols, 2 * n_deg))
    p_fwd = np.zeros((lat_devs, m_per, n_deg, lat_devs, row_pad))
    p_inv = np.zeros((lat_devs, m_per, lat_devs, row_pad, n_deg))
    for d in range(lat_devs):
        order = np.concatenate([(d ^ t) + lat_devs * np.arange(m_per) for t in range(lat_devs)])
        for h in range(lon_devs):
            for s in range(lon_devs):
                cut = slice((h ^ s) * cols, ((h ^ s) + 1) * cols)
                t_fwd[d, h, s] = fwd[order].reshape(2 * n_deg, n_lon)[:, cut]
                t_inv[d, h, s] = inv[order].reshape(2 * n_deg, n_lon)[:, cut].T
        mine = d + lat_devs * np.arange(m_per)
        for t in range(lat_devs):
            cut = slice((d ^ t) * rows, ((d ^ t) + 1) * rows)
            p_fwd[d, :, :, t, :rows] = leg_w[:, mine, cut].transpose(1, 0, 2)
            p_inv[d, :, t, :rows, :] = leg[:, mine, cut].transpose(1, 2, 0)
    p_fwd = p_fwd.reshape(lat_devs, m_per, n_deg, lat_devs * row_pad)
    p_inv = p_inv.reshape(lat_devs, m_per, lat_devs * row_pad, n_deg)
    return [np.asarray(np.asarray(x, np.float32), dtype=BF) for x in (t_fwd, t_inv, p_fwd, p_inv)]


def dot(a, b):
    return jnp.dot(a, b, preferred_element_type=F32)


def fourier_kernel(sp, f_ref, r_ref, t_ref, o0, o1, o2, o3, scr):
    outs = (o0, o1, o2, o3)
    k_n = r_ref.shape[0]
    m2 = t_ref.shape[3]
    per, row_pad = o0.shape[0], o0.shape[1]
    scr[pl.ds(k_n * m2, (row_pad - k_n) * m2), :] = jnp.zeros(((row_pad - k_n) * m2, LANE), F32)

    def step(p, _):
        k = jnp.minimum(2 * p, k_n - 2)
        mine = jnp.concatenate([f_ref[0, k], f_ref[0, k + 1]], axis=1).astype(BF)
        other = jnp.concatenate([r_ref[k], r_ref[k + 1]], axis=1)
        acc = dot(t_ref[0, 0, 0], mine) + dot(t_ref[0, 0, 1], other)
        base = pl.multiple_of(k * m2, 8)
        scr[pl.ds(base, m2), :] = acc[:, :LANE]
        scr[pl.ds(base + m2, m2), :] = acc[:, LANE:]
        return 0

    lax.fori_loop(0, (k_n + 1) // 2, step, 0)

    def spread(i, _):
        for t in range(4):
            outs[t][i] = scr[pl.ds(t * per + i, row_pad, stride=m2), :].astype(BF)
        return 0

    lax.fori_loop(0, per, spread, 0)


def analysis_kernel(sp, x0, x1, x2, x3, p_ref, o_ref, scr, *, stride):
    xs = (x0, x1, x2, x3)
    m_per, n_deg = p_ref.shape[1], p_ref.shape[2]
    m_pad = o_ref.shape[2]
    for r in range(2):
        scr[r, pl.ds(m_per * stride, (m_pad - m_per) * stride), :] = jnp.zeros(((m_pad - m_per) * stride, LANE), F32)

    def step(i, _):
        re = jnp.concatenate([x[2 * i] for x in xs], axis=0)
        im = jnp.concatenate([x[2 * i + 1] for x in xs], axis=0)
        acc = dot(p_ref[0, i], jnp.concatenate([re, im], axis=1))
        base = pl.multiple_of(i * stride, 8)
        scr[0, pl.ds(base, n_deg), :] = acc[:, :LANE]
        scr[1, pl.ds(base, n_deg), :] = acc[:, LANE:]
        return 0

    lax.fori_loop(0, m_per, step, 0)

    def spread(l, _):
        for r in range(2):
            o_ref[r, l] = scr[r, pl.ds(l, m_pad, stride=stride), :].astype(BF)
        return 0

    lax.fori_loop(0, n_deg, spread, 0)


def mixing_kernel(*refs, parts):
    a_refs, w_ref, o_refs = refs[:parts], refs[parts], refs[parts + 1:]
    cw = o_refs[0].shape[3]
    m_pad = o_refs[0].shape[2]

    def step(l, _):
        re = jnp.concatenate([a[0, l] for a in a_refs], axis=1)
        im = jnp.concatenate([a[1, l] for a in a_refs], axis=1)
        lhs = jnp.concatenate([jnp.concatenate([re, -im], axis=1), jnp.concatenate([im, re], axis=1)], axis=0)
        acc = dot(lhs, w_ref[l]).astype(BF)
        for j, o in enumerate(o_refs):
            o[0, l] = acc[:m_pad, j * cw:(j + 1) * cw]
            o[1, l] = acc[m_pad:, j * cw:(j + 1) * cw]
        return 0

    lax.fori_loop(0, w_ref.shape[0], step, 0)


def synthesis_kernel(sp, b_ref, p_ref, o0, o1, o2, o3, scr, *, stride):
    outs = (o0, o1, o2, o3)
    m_per, n_deg = p_ref.shape[1], p_ref.shape[3]
    m_pad = b_ref.shape[2]
    row_pad = o0.shape[1]

    def load(l, _):
        base = pl.multiple_of(l * stride, 8)
        for r in range(2):
            scr[r, pl.ds(base, m_pad), :] = b_ref[r, l].astype(F32)
        return 0

    lax.fori_loop(0, n_deg, load, 0)

    def step(i, _):
        x = jnp.concatenate([scr[r, pl.ds(i, n_deg, stride=stride), :] for r in range(2)], axis=1).astype(BF)
        acc = dot(p_ref[0, i], x).astype(BF)
        for t in range(4):
            outs[t][2 * i] = acc[t * row_pad:(t + 1) * row_pad, :LANE]
            outs[t][2 * i + 1] = acc[t * row_pad:(t + 1) * row_pad, LANE:]
        return 0

    lax.fori_loop(0, m_per, step, 0)


def inverse_kernel(sp, x0, x1, x2, x3, t_ref, own_ref, snd_ref, scr, *, stride):
    xs = (x0, x1, x2, x3)
    per, row_pad = x0.shape[0], x0.shape[1]
    k_n = own_ref.shape[0]

    def load(i, _):
        for t in range(4):
            base = pl.multiple_of((t * per + i) * stride, 8)
            scr[pl.ds(base, row_pad), :] = xs[t][i].astype(F32)
        return 0

    lax.fori_loop(0, per, load, 0)

    def step(p, _):
        k = jnp.minimum(2 * p, k_n - 2)
        x = jnp.concatenate([scr[pl.ds(k + e, 4 * per, stride=stride), :] for e in range(2)], axis=1).astype(BF)
        own = dot(t_ref[0, 0, 0], x).astype(BF)
        own_ref[k] = own[:, :LANE]
        own_ref[k + 1] = own[:, LANE:]
        snd = dot(t_ref[0, 0, 1], x).astype(BF)
        snd_ref[k] = snd[:, :LANE]
        snd_ref[k + 1] = snd[:, LANE:]
        return 0

    lax.fori_loop(0, (k_n + 1) // 2, step, 0)


def final_kernel(sp, f_ref, y_ref, *rest):
    out_ref = rest[-1]
    y = y_ref[...].astype(F32)
    out_ref[0] = f_ref[0] + 0.5 * y * (1.0 + lax.erf(y * (2.0 ** -0.5)))


def solution(mesh):
    lat_devs = mesh.shape['lat']
    lon_devs = mesh.shape['lon']

    def local_layer(grid_field, mix_weight):
        batch, chans, rows, cols = grid_field.shape
        n_lat, n_lon = rows * lat_devs, cols * lon_devs
        n_deg = mix_weight.shape[0]
        m_per = n_deg // lat_devs
        per = 2 * m_per
        pad = -(-rows // 16) * 16
        fields = batch // lon_devs
        cw = chans
        parts = chans // cw
        t_fwd, t_inv, p_fwd, p_inv = (jnp.asarray(x) for x in build_tables(n_lat, n_lon, n_deg, lat_devs, lon_devs, pad))
        lat = lax.axis_index('lat').astype(jnp.int32)
        lon = lax.axis_index('lon').astype(jnp.int32)
        field = grid_field.transpose(0, 2, 3, 1)
        weight = mix_weight.transpose(0, 3, 1, 2).reshape(n_deg, 2 * chans, chans)
        swap = [(0, 1), (1, 0)]
        vmem = pltpu.CompilerParams(vmem_limit_bytes=60 * 2 ** 20)

        def call(kernel, sp, grid, ins, outs, scratch, args, cost, aliases={}):
            return pl.pallas_call(
                kernel,
                grid_spec=pltpu.PrefetchScalarGridSpec(num_scalar_prefetch=1, grid=grid, in_specs=ins, out_specs=outs[1], scratch_shapes=scratch),
                out_shape=outs[0], compiler_params=vmem, input_output_aliases=aliases,
                cost_estimate=pl.CostEstimate(flops=cost, bytes_accessed=0, transcendentals=0))(sp, *args)

        spec_x = pl.BlockSpec((per, pad, LANE), lambda c, sp: (0, 0, c))
        shape_x = jax.ShapeDtypeStruct((per, pad, cw), BF)
        shape_y = jax.ShapeDtypeStruct((rows, cols, cw), BF)
        spec_y = pl.BlockSpec((rows, cols, LANE), lambda c, sp: (0, 0, c))
        spec_s = pl.BlockSpec((2, n_deg, pad, LANE), lambda c, sp: (0, 0, 0, c))
        shape_s = jax.ShapeDtypeStruct((2, n_deg, pad, cw), BF)
        spec_t = lambda a, b: pl.BlockSpec((1, 1, lon_devs, a, b), lambda c, sp: (sp[1], sp[2], 0, 0, 0))
        spec_p = lambda a, b: pl.BlockSpec((1, m_per, a, b), lambda c, sp: (sp[1], 0, 0, 0))
        n_blk = cw // LANE
        unit = int(1e9)

        def lat_swap(xs):
            return [xs[0]] + [lax.ppermute(xs[t], 'lat', [(s, s ^ t) for s in range(lat_devs)]) for t in range(1, lat_devs)]

        out = None
        spectral = []
        sps = [jnp.stack([lon * fields + q, lat, lon, (1 - lon) * fields + q]) for q in range(fields)]
        received = []
        for q in range(fields):
            send = lax.dynamic_index_in_dim(field, (1 - lon) * fields + q, 0, keepdims=False).astype(BF)
            received.append(lax.ppermute(send, 'lon', swap))
        for q in range(fields):
            sp = sps[q]
            xs = call(fourier_kernel, sp, (n_blk,),
                      [pl.BlockSpec((1, rows, cols, LANE), lambda c, sp: (sp[0], 0, 0, c)), spec_y, spec_t(2 * n_deg, cols)],
                      ([shape_x] * 4, [spec_x] * 4), [pltpu.VMEM((pad * 2 * n_deg, LANE), F32)],
                      (field, received[q], t_fwd), 20 * unit)
            xs = lat_swap(xs)
            st = -(-n_deg // 8) * 8
            spectral.append(call(functools.partial(analysis_kernel, stride=st), sp, (n_blk,),
                                 [spec_x] * 4 + [spec_p(n_deg, lat_devs * pad)],
                                 (shape_s, spec_s), [pltpu.VMEM((2, pad * st, LANE), F32)],
                                 (*xs, p_fwd), 20 * unit))
        blk = 6
        own_y, got_y = [], []
        for q in range(fields):
            sp = sps[q]
            mixed = pl.pallas_call(
                functools.partial(mixing_kernel, parts=parts), grid=(n_deg // blk,),
                in_specs=[pl.BlockSpec((2, blk, pad, cw), lambda l: (0, l, 0, 0))] * parts + [pl.BlockSpec((blk, 2 * chans, chans), lambda l: (l, 0, 0))],
                out_specs=[pl.BlockSpec((2, blk, pad, cw), lambda l: (0, l, 0, 0))] * parts,
                out_shape=[shape_s] * parts, compiler_params=vmem,
                cost_estimate=pl.CostEstimate(flops=40 * unit, bytes_accessed=0, transcendentals=0))(spectral[q], weight)
            xs = call(functools.partial(synthesis_kernel, stride=56), sp, (n_blk,),
                      [spec_s, spec_p(lat_devs * pad, n_deg)], ([shape_x] * 4, [spec_x] * 4),
                      [pltpu.VMEM((2, n_deg * 56, LANE), F32)], (mixed[0], p_inv), 20 * unit)
            xs = lat_swap(xs)
            own, snd = call(functools.partial(inverse_kernel, stride=56), sp, (n_blk,),
                            [spec_x] * 4 + [spec_t(cols, 2 * n_deg)], ([shape_y] * 2, [spec_y] * 2),
                            [pltpu.VMEM((4 * per * 56, LANE), F32)], (*xs, t_inv), 20 * unit)
            own_y.append(own)
            got_y.append(lax.ppermute(snd, 'lon', swap))
        kb = 9
        out_shape = jax.ShapeDtypeStruct(field.shape, F32)

        def finish(out, y, q, which):
            fspec = pl.BlockSpec((1, kb, cols, LANE), lambda k, c, sp: (sp[which], k, 0, c))
            ins = [fspec, pl.BlockSpec((kb, cols, LANE), lambda k, c, sp: (k, 0, c))]
            args = [field, y]
            aliases = {}
            if out is not None:
                ins.append(pl.BlockSpec(memory_space=pl.ANY))
                args.append(out)
                aliases = {3: 0}
            return call(final_kernel, sps[q], (rows // kb, n_blk), ins, (out_shape, fspec), [], args, 8 * unit, aliases)

        for q in range(fields):
            out = finish(out, own_y[q], q, 0)
        for q in range(fields):
            out = finish(out, got_y[q], q, 3)
        return out.transpose(0, 3, 1, 2)

    field_spec = P('member', None, 'lat', 'lon')
    return jax.shard_map(local_layer, mesh=mesh, in_specs=(field_spec, P()), out_specs=field_spec, check_vma=False)
```
